32 devices in a mesh: section: 2 (over x), outer: 4 (over y, core), tensor: 4 (over z).
Axes of the slice: x: 2, y: 2, z: 4, core: 2. Of those that a mesh axis runs over, the one named last changes fastest.
Arguments:
- act_in: bfloat16 [2, 16, 8192], P('section', 'outer', 'tensor'), may hold values from -6 to 6
- saved_in: bfloat16 [2, 16, 8192], P('section', 'outer', 'tensor'), may hold values from -6 to 6
- cotangent: bfloat16 [2, 16, 8192], P('section', 'outer', 'tensor'), may hold values from -6 to 6
- w_gate: bfloat16 [2, 8192, 14336], P('section', 'tensor', 'outer'), may hold values from -0.0625 to 0.0625
- w_up: bfloat16 [2, 8192, 14336], P('section', 'tensor', 'outer'), may hold values from -0.0625 to 0.0625
- w_down: bfloat16 [2, 14336, 8192], P('section', 'outer', 'tensor'), may hold values from -0.046875 to 0.046875
Outputs:
- forward_sent: bfloat16 [2, 16, 8192], P('section', 'outer', 'tensor')
- grad_sent: bfloat16 [2, 16, 8192], P('section', 'outer', 'tensor')
The draws below stay inside these ranges and needn't reach their ends.
All inputs are finite; a program needn't handle non-finite values.
Results may differ from the reference program's by a relative error of at most 0.025.
Values may be sent and summed in bfloat16 or wider, within the bound.
A program may use at most 128 MiB of HBM per device.

```python
import jax
import jax.numpy as jnp
from jax import lax

D = 8192
H = 14336
CELL_ROWS = 1
GROUPS = 4
TOKENS = 16
D_BLOCK = 2048
N_TENSOR = 4


def levels(rng, extent, cuts, least, largest):
    factor_of = 1.0
    for axis_at, blocks in cuts:
        draws = jax.random.uniform(jax.random.fold_in(jax.random.fold_in(rng, 6), axis_at), (blocks,), jnp.float32, least / len(cuts), largest / len(cuts))
        factor_of = factor_of * jnp.repeat(jnp.exp(draws), extent[axis_at] // blocks).reshape((-1,) + (1,) * (len(extent) - 1 - axis_at))
    return factor_of


def bell_draw(stream_key, shape, width, reach, cuts=(), kind=jnp.bfloat16):
    gain = levels(stream_key, shape, cuts, -0.22, 0.18) if cuts else 1.0
    drawn = jax.random.normal(stream_key, shape, jnp.float32) * width * gain
    return jnp.minimum(jnp.maximum(drawn, -reach), reach).astype(kind)


def setup_inputs(seed: int = 0) -> dict:
    arg_keys = jax.random.split(jax.random.key(seed), 7)
    act_in = bell_draw(arg_keys[0], (2, TOKENS, D), 1.0, 6.0, ((0, 2), (1, 4), (2, 4)))
    saved_in = bell_draw(arg_keys[1], (2, TOKENS, D), 1.0, 6.0, ((0, 2), (1, 4), (2, 4)))
    cotangent = bell_draw(arg_keys[2], (2, TOKENS, D), 1.0, 6.0, ((0, 2), (1, 4), (2, 4)))
    w_gate = bell_draw(arg_keys[3], (2, D, H), D ** -0.5, 0.0625, ((0, 2), (1, 4), (2, 4)))
    w_up = bell_draw(arg_keys[4], (2, D, H), D ** -0.5, 0.0625, ((0, 2), (1, 4), (2, 4)))
    w_down = bell_draw(arg_keys[5], (2, H, D), H ** -0.5, 0.046875, ((0, 2), (1, 4), (2, 4)))
    return dict(act_in=act_in, saved_in=saved_in, cotangent=cotangent, w_gate=w_gate, w_up=w_up, w_down=w_down)


def reorder(matrix):
    return matrix.reshape(GROUPS, GROUPS, CELL_ROWS, matrix.shape[1]).transpose(1, 0, 2, 3).reshape(matrix.shape)


def rounded(product):
    return lax.optimization_barrier(product.astype(jnp.bfloat16)).astype(jnp.float32)


def block_sum(left, right):
    left_blocks = left.reshape(TOKENS, N_TENSOR, D_BLOCK).transpose(1, 0, 2)
    right_blocks = right.reshape(N_TENSOR, D_BLOCK, right.shape[1])

    def add_block(running, pieces):
        partial_value = jnp.dot(pieces[0], pieces[1], preferred_element_type=jnp.float32)
        return running + rounded(partial_value), None

    begin_sum = jnp.zeros((TOKENS, right.shape[1]), jnp.float32)
    result, unused = lax.scan(add_block, begin_sum, (left_blocks, right_blocks))
    return result


def section_math(current, stored, incoming, gate_mat, up_mat, down_mat):
    gate_pre = block_sum(current, gate_mat)
    up_pre = block_sum(current, up_mat)
    hidden = (jax.nn.silu(gate_pre) * up_pre).astype(jnp.bfloat16)
    output = (current.astype(jnp.float32) + jnp.dot(hidden, down_mat, preferred_element_type=jnp.float32)).astype(jnp.bfloat16)
    gate_saved = block_sum(stored, gate_mat)
    up_saved = block_sum(stored, up_mat)
    hidden_grad = block_sum(incoming, down_mat.T)
    squash = jax.nn.sigmoid(gate_saved)
    gate_grad = (hidden_grad * up_saved * squash * (1.0 + gate_saved * (1.0 - squash))).astype(jnp.bfloat16)
    up_grad = (hidden_grad * gate_saved * squash).astype(jnp.bfloat16)
    backward = jnp.dot(gate_grad, gate_mat.T, preferred_element_type=jnp.float32) + jnp.dot(up_grad, up_mat.T, preferred_element_type=jnp.float32)
    input_grad = (incoming.astype(jnp.float32) + backward).astype(jnp.bfloat16)
    return output, input_grad


def reference(act_in, saved_in, cotangent, w_gate, w_up, w_down):
    first = section_math(act_in[0], saved_in[0], cotangent[0], w_gate[0], w_up[0], w_down[0])
    second = section_math(act_in[1], saved_in[1], cotangent[1], w_gate[1], w_up[1], w_down[1])
    forward_sent = jnp.stack([reorder(second[0]), reorder(first[0])])
    grad_sent = jnp.stack([reorder(second[1]), reorder(first[1])])
    return forward_sent, grad_sent
```

```python
import functools

import jax
import jax.numpy as jnp
from jax import lax
from jax.experimental import pallas as pl
from jax.experimental.pallas import tpu as pltpu
from jax.sharding import PartitionSpec as P

MESH = pl.DeviceIdType.MESH
F32 = jnp.float32
BF16 = jnp.bfloat16
CONTRACT_LAST = (((1,), (1,)), ((), ()))
SUM_LAG = 2
SECOND_LAG = 4


def kernel(
    sections, outers, tensors, chunks, chunk,
    act, saved, cot, w_gate, w_up, w_down,
    out_ref, grad_ref,
    gate_buf, up_buf, down_buf, gathered, staging, rows_f32, lhs_two, lhs_cot,
    products, part, arrived, shared, second_f32, total, final_out, final_in,
    load_sem, weight_sem, gather_send, gather_recv, part_send, part_recv,
    share_send, share_recv, final_send, final_recv,
):
    section = lax.axis_index("section")
    outer = lax.axis_index("outer")
    tensor = lax.axis_index("tensor")
    other = lax.rem(section + 1, sections)
    own_rows = act.shape[1]
    rows = own_rows * outers
    cells = own_rows // outers
    shard = rows // tensors

    loads = [
        pltpu.make_async_copy(source.at[0], gathered.at[which, outer], load_sem.at[which])
        for which, source in enumerate((act, saved, cot))
    ]
    for load in loads:
        load.start()

    def weight_copies(c):
        span = pl.ds(pl.multiple_of(c * chunk, chunk), chunk)
        return (
            pltpu.make_async_copy(w_gate.at[0, :, span], gate_buf.at[c], weight_sem.at[0, c]),
            pltpu.make_async_copy(w_up.at[0, :, span], up_buf.at[c], weight_sem.at[1, c]),
            pltpu.make_async_copy(w_down.at[0, span, :], down_buf.at[c], weight_sem.at[2, c]),
        )

    for c in range(chunks):
        for copy in weight_copies(c):
            copy.start()

    barrier = pltpu.get_barrier_semaphore()
    for step in range(1, outers):
        pl.semaphore_signal(
            barrier, 1, device_id={"outer": lax.rem(outer + step, outers)}, device_id_type=MESH
        )
    for step in range(1, tensors):
        pl.semaphore_signal(
            barrier, 1, device_id={"tensor": lax.rem(tensor + step, tensors)}, device_id_type=MESH
        )
    for place in range(outers):
        pl.semaphore_signal(
            barrier, 1, device_id={"section": other, "outer": place}, device_id_type=MESH
        )
    pl.semaphore_wait(barrier, 2 * outers + tensors - 2)

    def gather_copy(which, origin, target):
        return pltpu.make_async_remote_copy(
            src_ref=gathered.at[which, origin],
            dst_ref=gathered.at[which, origin],
            send_sem=gather_send.at[which, target],
            recv_sem=gather_recv.at[which, origin],
            device_id={"outer": target},
            device_id_type=MESH,
        )

    for which in range(3):
        loads[which].wait()
        for step in range(1, outers):
            gather_copy(which, outer, lax.rem(outer + step, outers)).start()

    for which in range(3):
        for step in range(1, outers):
            origin = lax.rem(outer + step, outers)
            gather_copy(which, origin, origin).wait_recv()
        for origin in range(outers):
            staging[...] = gathered[which, origin].astype(F32)
            for j in range(outers):
                to = (j * outers + origin) * cells
                rows_f32[which, to : to + cells, :] = staging[j * cells : (j + 1) * cells, :]
    lhs_two[0:rows, :] = rows_f32[0].astype(BF16)
    lhs_two[rows : 2 * rows, :] = rows_f32[1].astype(BF16)
    lhs_cot[...] = rows_f32[2].astype(BF16)
    place = lax.broadcasted_iota(jnp.int32, total.shape[1:], 0)
    mine = lax.rem(lax.div(place, cells), outers) == outer
    total[0] = jnp.where(mine, rows_f32[0], 0.0)
    total[1] = jnp.where(mine, rows_f32[2], 0.0)

    def part_copy(c, origin, target):
        return pltpu.make_async_remote_copy(
            src_ref=part.at[c, target],
            dst_ref=arrived.at[c, origin],
            send_sem=part_send.at[c, target],
            recv_sem=part_recv.at[c, origin],
            device_id={"tensor": target},
            device_id_type=MESH,
        )

    def share_copy(c, origin, target):
        return pltpu.make_async_remote_copy(
            src_ref=shared.at[c, origin],
            dst_ref=shared.at[c, origin],
            send_sem=share_send.at[c, target],
            recv_sem=share_recv.at[c, origin],
            device_id={"tensor": target},
            device_id_type=MESH,
        )

    def first(c):
        for copy in weight_copies(c):
            copy.wait()
        two = lhs_two[...]
        products[0 : 2 * rows, :] = jnp.dot(two, gate_buf[c], preferred_element_type=F32)
        products[2 * rows : 4 * rows, :] = jnp.dot(two, up_buf[c], preferred_element_type=F32)
        products[4 * rows : 5 * rows, :] = lax.dot_general(
            lhs_cot[...], down_buf[c], CONTRACT_LAST, preferred_element_type=F32
        )
        for target in range(tensors):
            for which in range(5):
                part[c, target, which] = products[
                    which * rows + target * shard : which * rows + (target + 1) * shard, :
                ].astype(BF16)
        for step in range(1, tensors):
            part_copy(c, tensor, lax.rem(tensor + step, tensors)).start()

    def combine(c):
        for step in range(1, tensors):
            origin = lax.rem(tensor + step, tensors)
            part_copy(c, origin, origin).wait_recv()
        sums = []
        for which in range(5):
            summed = part[c, tensor, which].astype(F32)
            for step in range(1, tensors):
                summed = summed + arrived[c, lax.rem(tensor + step, tensors), which].astype(F32)
            sums.append(summed)
        gate_pre, gate_saved, up_pre, up_saved, hidden_grad = sums
        squash = jax.nn.sigmoid(gate_saved)
        shared[c, tensor, 0] = (gate_pre * jax.nn.sigmoid(gate_pre) * up_pre).astype(BF16)
        shared[c, tensor, 1] = (
            hidden_grad * up_saved * squash * (1.0 + gate_saved * (1.0 - squash))
        ).astype(BF16)
        shared[c, tensor, 2] = (hidden_grad * gate_saved * squash).astype(BF16)
        for step in range(1, tensors):
            share_copy(c, tensor, lax.rem(tensor + step, tensors)).start()

    def second(c):
        for step in range(1, tensors):
            origin = lax.rem(tensor + step, tensors)
            share_copy(c, origin, origin).wait_recv()
        for origin in range(tensors):
            for which in range(3):
                second_f32[which, origin * shard : (origin + 1) * shard, :] = shared[
                    c, origin, which
                ].astype(F32)
        total[0] += jnp.dot(
            second_f32[0].astype(BF16), down_buf[c], preferred_element_type=F32
        )
        total[1] += lax.dot_general(
            second_f32[1].astype(BF16), gate_buf[c], CONTRACT_LAST, preferred_element_type=F32
        ) + lax.dot_general(
            second_f32[2].astype(BF16), up_buf[c], CONTRACT_LAST, preferred_element_type=F32
        )

    def advance(step, carry):
        @pl.when(step < chunks)
        def _():
            first(step)

        @pl.when((step >= SUM_LAG) & (step < chunks + SUM_LAG))
        def _():
            combine(step - SUM_LAG)

        @pl.when(step >= SECOND_LAG)
        def _():
            second(step - SECOND_LAG)

        return carry

    lax.fori_loop(0, chunks + SECOND_LAG, advance, 0)

    def final_copy(origin, target):
        return pltpu.make_async_remote_copy(
            src_ref=final_out.at[target],
            dst_ref=final_in.at[origin],
            send_sem=final_send.at[target],
            recv_sem=final_recv.at[origin],
            device_id={"section": other, "outer": target},
            device_id_type=MESH,
        )

    for target in range(outers):
        for which in range(2):
            final_out[target, which] = total[
                which, target * own_rows : (target + 1) * own_rows, :
            ].astype(BF16)
        final_copy(outer, target).start()

    def drain(c, carry):
        for step in range(1, tensors):
            target = lax.rem(tensor + step, tensors)
            part_copy(c, tensor, target).wait_send()
            share_copy(c, tensor, target).wait_send()
        return carry

    lax.fori_loop(0, chunks, drain, 0)
    for which in range(3):
        for step in range(1, outers):
            gather_copy(which, outer, lax.rem(outer + step, outers)).wait_send()

    for origin in range(outers):
        final_copy(origin, origin).wait_recv()
    for which, result in enumerate((out_ref, grad_ref)):
        summed = final_in[0, which].astype(F32)
        for origin in range(1, outers):
            summed = summed + final_in[origin, which].astype(F32)
        result[0] = summed.astype(BF16)
    for target in range(outers):
        final_copy(outer, target).wait_send()


def solution(mesh):
    sections, outers, tensors = (mesh.shape[name] for name in ("section", "outer", "tensor"))

    def on_device(act_in, saved_in, cotangent, w_gate, w_up, w_down):
        own_rows, model_width = act_in.shape[1:]
        width = w_gate.shape[2]
        rows = own_rows * outers
        shard = rows // tensors
        chunk = next(size for size in (512, 256, 128, width) if width % size == 0)
        chunks = width // chunk
        dma = pltpu.SemaphoreType.DMA
        out = jax.ShapeDtypeStruct((1, own_rows, model_width), BF16)
        return pl.pallas_call(
            functools.partial(kernel, sections, outers, tensors, chunks, chunk),
            out_shape=(out, out),
            in_specs=[pl.BlockSpec(memory_space=pl.ANY)] * 6,
            out_specs=[pl.BlockSpec(memory_space=pltpu.VMEM)] * 2,
            scratch_shapes=[
                pltpu.VMEM((chunks, model_width, chunk), BF16),
                pltpu.VMEM((chunks, model_width, chunk), BF16),
                pltpu.VMEM((chunks, chunk, model_width), BF16),
                pltpu.VMEM((3, outers, own_rows, model_width), BF16),
                pltpu.VMEM((own_rows, model_width), F32),
                pltpu.VMEM((3, rows, model_width), F32),
                pltpu.VMEM((2 * rows, model_width), BF16),
                pltpu.VMEM((rows, model_width), BF16),
                pltpu.VMEM((5 * rows, chunk), F32),
                pltpu.VMEM((chunks, tensors, 5, shard, chunk), BF16),
                pltpu.VMEM((chunks, tensors, 5, shard, chunk), BF16),
                pltpu.VMEM((chunks, tensors, 3, shard, chunk), BF16),
                pltpu.VMEM((3, rows, chunk), F32),
                pltpu.VMEM((2, rows, model_width), F32),
                pltpu.VMEM((outers, 2, own_rows, model_width), BF16),
                pltpu.VMEM((outers, 2, own_rows, model_width), BF16),
                dma((3,)),
                dma((3, chunks)),
                dma((3, outers)),
                dma((3, outers)),
                dma((chunks, tensors)),
                dma((chunks, tensors)),
                dma((chunks, tensors)),
                dma((chunks, tensors)),
                dma((outers,)),
                dma((outers,)),
            ],
            compiler_params=pltpu.CompilerParams(
                collective_id=0, has_side_effects=True, vmem_limit_bytes=60 * 1024 * 1024
            ),
        )(act_in, saved_in, cotangent, w_gate, w_up, w_down)

    return jax.shard_map(
        on_device,
        mesh=mesh,
        in_specs=(
            P("section", "outer", "tensor"),
            P("section", "outer", "tensor"),
            P("section", "outer", "tensor"),
            P("section", "tensor", "outer"),
            P("section", "tensor", "outer"),
            P("section", "outer", "tensor"),
        ),
        out_specs=(P("section", "outer", "tensor"), P("section", "outer", "tensor")),
        check_vma=False,
    )
```

```python
import functools

import jax
import jax.numpy as jnp
from jax import lax
from jax.experimental import pallas as pl
from jax.experimental.pallas import tpu as pltpu
from jax.sharding import PartitionSpec as P

MESH = pl.DeviceIdType.MESH
F32 = jnp.float32
BF16 = jnp.bfloat16
CONTRACT_LAST = (((1,), (1,)), ((), ()))
SUM_LAG = 2
SECOND_LAG = 4
AHEAD = 2


def kernel(
    sections, outers, tensors, chunks, chunk,
    act, saved, cot, w_gate, w_up, w_down,
    out_ref, grad_ref,
    gate_buf, up_buf, down_buf, gathered, staging, rows_f32, lhs_two, lhs_cot,
    products, part, arrived, shared, second_f32, total, final_out, final_in,
    load_sem, weight_sem, gather_send, gather_recv, part_send, part_recv,
    share_send, share_recv, final_send, final_recv,
):
    section = lax.axis_index("section")
    outer = lax.axis_index("outer")
    tensor = lax.axis_index("tensor")
    other = lax.rem(section + 1, sections)
    own_rows = act.shape[1]
    rows = own_rows * outers
    cells = own_rows // outers
    shard = rows // tensors

    loads = [
        pltpu.make_async_copy(source.at[0], gathered.at[which, outer], load_sem.at[which])
        for which, source in enumerate((act, saved, cot))
    ]
    for load in loads:
        load.start()

    def weight_copies(c):
        span = pl.ds(pl.multiple_of(c * chunk, chunk), chunk)
        return (
            pltpu.make_async_copy(w_gate.at[0, :, span], gate_buf.at[c], weight_sem.at[0, c]),
            pltpu.make_async_copy(w_up.at[0, :, span], up_buf.at[c], weight_sem.at[1, c]),
            pltpu.make_async_copy(w_down.at[0, span, :], down_buf.at[c], weight_sem.at[2, c]),
        )

    for c in range(min(AHEAD, chunks)):
        for copy in weight_copies(c):
            copy.start(priority=1)

    barrier = pltpu.get_barrier_semaphore()
    for step in range(1, outers):
        pl.semaphore_signal(
            barrier, 1, device_id={"outer": lax.rem(outer + step, outers)}, device_id_type=MESH
        )
    for step in range(1, tensors):
        pl.semaphore_signal(
            barrier, 1, device_id={"tensor": lax.rem(tensor + step, tensors)}, device_id_type=MESH
        )
    for place in range(outers):
        pl.semaphore_signal(
            barrier, 1, device_id={"section": other, "outer": place}, device_id_type=MESH
        )
    pl.semaphore_wait(barrier, 2 * outers + tensors - 2)

    def gather_copy(which, origin, target):
        return pltpu.make_async_remote_copy(
            src_ref=gathered.at[which, origin],
            dst_ref=gathered.at[which, origin],
            send_sem=gather_send.at[which, target],
            recv_sem=gather_recv.at[which, origin],
            device_id={"outer": target},
            device_id_type=MESH,
        )

    for which in range(3):
        loads[which].wait()
        for step in range(1, outers):
            gather_copy(which, outer, lax.rem(outer + step, outers)).start()

    for which in range(3):
        for step in range(1, outers):
            origin = lax.rem(outer + step, outers)
            gather_copy(which, origin, origin).wait_recv()
        for origin in range(outers):
            staging[...] = gathered[which, origin].astype(F32)
            for j in range(outers):
                to = (j * outers + origin) * cells
                rows_f32[which, to : to + cells, :] = staging[j * cells : (j + 1) * cells, :]
    lhs_two[0:rows, :] = rows_f32[0].astype(BF16)
    lhs_two[rows : 2 * rows, :] = rows_f32[1].astype(BF16)
    lhs_cot[...] = rows_f32[2].astype(BF16)
    place = lax.broadcasted_iota(jnp.int32, total.shape[1:], 0)
    mine = lax.rem(lax.div(place, cells), outers) == outer
    total[0] = jnp.where(mine, rows_f32[0], 0.0)
    total[1] = jnp.where(mine, rows_f32[2], 0.0)

    def part_copy(c, origin, target):
        return pltpu.make_async_remote_copy(
            src_ref=part.at[c, target],
            dst_ref=arrived.at[c, origin],
            send_sem=part_send.at[c, target],
            recv_sem=part_recv.at[c, origin],
            device_id={"tensor": target},
            device_id_type=MESH,
        )

    def share_copy(c, origin, target):
        return pltpu.make_async_remote_copy(
            src_ref=shared.at[c, origin],
            dst_ref=shared.at[c, origin],
            send_sem=share_send.at[c, target],
            recv_sem=share_recv.at[c, origin],
            device_id={"tensor": target},
            device_id_type=MESH,
        )

    def first(c):
        @pl.when(c + AHEAD < chunks)
        def _():
            for copy in weight_copies(c + AHEAD):
                copy.start(priority=1)

        for copy in weight_copies(c):
            copy.wait()
        two = lhs_two[...]
        products[0 : 2 * rows, :] = jnp.dot(two, gate_buf[c], preferred_element_type=F32)
        products[2 * rows : 4 * rows, :] = jnp.dot(two, up_buf[c], preferred_element_type=F32)
        products[4 * rows : 5 * rows, :] = lax.dot_general(
            lhs_cot[...], down_buf[c], CONTRACT_LAST, preferred_element_type=F32
        )
        for target in range(tensors):
            for which in range(5):
                part[c, target, which] = products[
                    which * rows + target * shard : which * rows + (target + 1) * shard, :
                ].astype(BF16)
        for step in range(1, tensors):
            part_copy(c, tensor, lax.rem(tensor + step, tensors)).start()

    def combine(c):
        for step in range(1, tensors):
            origin = lax.rem(tensor + step, tensors)
            part_copy(c, origin, origin).wait_recv()
        sums = []
        for which in range(5):
            summed = part[c, tensor, which].astype(F32)
            for step in range(1, tensors):
                summed = summed + arrived[c, lax.rem(tensor + step, tensors), which].astype(F32)
            sums.append(summed)
        gate_pre, gate_saved, up_pre, up_saved, hidden_grad = sums
        squash = jax.nn.sigmoid(gate_saved)
        shared[c, tensor, 0] = (gate_pre * jax.nn.sigmoid(gate_pre) * up_pre).astype(BF16)
        shared[c, tensor, 1] = (
            hidden_grad * up_saved * squash * (1.0 + gate_saved * (1.0 - squash))
        ).astype(BF16)
        shared[c, tensor, 2] = (hidden_grad * gate_saved * squash).astype(BF16)
        for step in range(1, tensors):
            share_copy(c, tensor, lax.rem(tensor + step, tensors)).start()

    def second(c):
        for step in range(1, tensors):
            origin = lax.rem(tensor + step, tensors)
            share_copy(c, origin, origin).wait_recv()
        for origin in range(tensors):
            for which in range(3):
                second_f32[which, origin * shard : (origin + 1) * shard, :] = shared[
                    c, origin, which
                ].astype(F32)
        total[0] += jnp.dot(
            second_f32[0].astype(BF16), down_buf[c], preferred_element_type=F32
        )
        total[1] += lax.dot_general(
            second_f32[1].astype(BF16), gate_buf[c], CONTRACT_LAST, preferred_element_type=F32
        ) + lax.dot_general(
            second_f32[2].astype(BF16), up_buf[c], CONTRACT_LAST, preferred_element_type=F32
        )

    def advance(step, carry):
        @pl.when(step < chunks)
        def _():
            first(step)

        @pl.when((step >= SUM_LAG) & (step < chunks + SUM_LAG))
        def _():
            combine(step - SUM_LAG)

        @pl.when(step >= SECOND_LAG)
        def _():
            second(step - SECOND_LAG)

        return carry

    lax.fori_loop(0, chunks + SECOND_LAG, advance, 0)

    def final_copy(origin, target):
        return pltpu.make_async_remote_copy(
            src_ref=final_out.at[target],
            dst_ref=final_in.at[origin],
            send_sem=final_send.at[target],
            recv_sem=final_recv.at[origin],
            device_id={"section": other, "outer": target},
            device_id_type=MESH,
        )

    for target in range(outers):
        for which in range(2):
            final_out[target, which] = total[
                which, target * own_rows : (target + 1) * own_rows, :
            ].astype(BF16)
        final_copy(outer, target).start()

    def drain(c, carry):
        for step in range(1, tensors):
            target = lax.rem(tensor + step, tensors)
            part_copy(c, tensor, target).wait_send()
            share_copy(c, tensor, target).wait_send()
        return carry

    lax.fori_loop(0, chunks, drain, 0)
    for which in range(3):
        for step in range(1, outers):
            gather_copy(which, outer, lax.rem(outer + step, outers)).wait_send()

    for origin in range(outers):
        final_copy(origin, origin).wait_recv()
    for which, result in enumerate((out_ref, grad_ref)):
        summed = final_in[0, which].astype(F32)
        for origin in range(1, outers):
            summed = summed + final_in[origin, which].astype(F32)
        result[0] = summed.astype(BF16)
    for target in range(outers):
        final_copy(outer, target).wait_send()


def solution(mesh):
    sections, outers, tensors = (mesh.shape[name] for name in ("section", "outer", "tensor"))

    def on_device(act_in, saved_in, cotangent, w_gate, w_up, w_down):
        own_rows, model_width = act_in.shape[1:]
        width = w_gate.shape[2]
        rows = own_rows * outers
        shard = rows // tensors
        chunk = next(size for size in (512, 256, 128, width) if width % size == 0)
        chunks = width // chunk
        dma = pltpu.SemaphoreType.DMA
        out = jax.ShapeDtypeStruct((1, own_rows, model_width), BF16)
        return pl.pallas_call(
            functools.partial(kernel, sections, outers, tensors, chunks, chunk),
            out_shape=(out, out),
            in_specs=[pl.BlockSpec(memory_space=pl.ANY)] * 6,
            out_specs=[pl.BlockSpec(memory_space=pltpu.VMEM)] * 2,
            scratch_shapes=[
                pltpu.VMEM((chunks, model_width, chunk), BF16),
                pltpu.VMEM((chunks, model_width, chunk), BF16),
                pltpu.VMEM((chunks, chunk, model_width), BF16),
                pltpu.VMEM((3, outers, own_rows, model_width), BF16),
                pltpu.VMEM((own_rows, model_width), F32),
                pltpu.VMEM((3, rows, model_width), F32),
                pltpu.VMEM((2 * rows, model_width), BF16),
                pltpu.VMEM((rows, model_width), BF16),
                pltpu.VMEM((5 * rows, chunk), F32),
                pltpu.VMEM((chunks, tensors, 5, shard, chunk), BF16),
                pltpu.VMEM((chunks, tensors, 5, shard, chunk), BF16),
                pltpu.VMEM((chunks, tensors, 3, shard, chunk), BF16),
                pltpu.VMEM((3, rows, chunk), F32),
                pltpu.VMEM((2, rows, model_width), F32),
                pltpu.VMEM((outers, 2, own_rows, model_width), BF16),
                pltpu.VMEM((outers, 2, own_rows, model_width), BF16),
                dma((3,)),
                dma((3, chunks)),
                dma((3, outers)),
                dma((3, outers)),
                dma((chunks, tensors)),
                dma((chunks, tensors)),
                dma((chunks, tensors)),
                dma((chunks, tensors)),
                dma((outers,)),
                dma((outers,)),
            ],
            compiler_params=pltpu.CompilerParams(
                collective_id=0, has_side_effects=True, vmem_limit_bytes=60 * 1024 * 1024
            ),
        )(act_in, saved_in, cotangent, w_gate, w_up, w_down)

    return jax.shard_map(
        on_device,
        mesh=mesh,
        in_specs=(
            P("section", "outer", "tensor"),
            P("section", "outer", "tensor"),
            P("section", "outer", "tensor"),
            P("section", "tensor", "outer"),
            P("section", "tensor", "outer"),
            P("section", "outer", "tensor"),
        ),
        out_specs=(P("section", "outer", "tensor"), P("section", "outer", "tensor")),
        check_vma=False,
    )
```
